8 devices in a mesh: datb: 2 (over z, y), model: 2 (over x), data: 2 (over core).
Axes of the slice: x: 2, y: 2, z: 1, core: 2. Of those that a mesh axis runs over, the one named last changes fastest.
Arguments:
- tokens: bfloat16 [4096, 4096], P(('datb', 'data', 'model'))
- w_gate: bfloat16 [4096, 14336], P(('datb', 'data'), 'model')
- w_up: bfloat16 [4096, 14336], P(('datb', 'data'), 'model')
- w_down: bfloat16 [14336, 4096], P('model', ('datb', 'data'))
- grad_out: bfloat16 [4096, 4096], P(('datb', 'data', 'model'))
Outputs:
- output 1: bfloat16 [4096, 4096], P(('datb', 'data', 'model'))
- output 2: bfloat16 [4096, 4096], P(('datb', 'data', 'model'))
- output 3: float32 [4096, 14336], P(('datb', 'data'), 'model')
- output 4: float32 [4096, 14336], P(('datb', 'data'), 'model')
- output 5: float32 [14336, 4096], P('model', ('datb', 'data'))
All inputs are finite; a program needn't handle non-finite values.
Results may differ from the reference program's by a relative error of at most 0.0160345.
Values are sent between devices in bfloat16 or wider.
A program may use at most 1 GiB of HBM per device.

```python
import jax
import jax.numpy as jnp
from jax import lax

D_MODEL = 4096
D_FF = 14336
TOKENS = 4096
BLOCK_ROWS = 512


def setup_inputs(seed: int = 0) -> dict:
    key = jax.random.key(seed)
    k_tok, k_gate, k_up, k_down, k_grad = jax.random.split(key, 5)
    tokens = jax.random.normal(k_tok, (TOKENS, D_MODEL), jnp.float32)
    w_gate = jax.random.normal(k_gate, (D_MODEL, D_FF), jnp.float32) * (D_MODEL ** -0.5)
    w_up = jax.random.normal(k_up, (D_MODEL, D_FF), jnp.float32) * (D_MODEL ** -0.5)
    w_down = jax.random.normal(k_down, (D_FF, D_MODEL), jnp.float32) * (1.5 * D_FF ** -0.5)
    grad_out = jax.random.normal(k_grad, (TOKENS, D_MODEL), jnp.float32)
    return {"tokens": tokens.astype(jnp.bfloat16), "w_gate": w_gate.astype(jnp.bfloat16), "w_up": w_up.astype(jnp.bfloat16), "w_down": w_down.astype(jnp.bfloat16), "grad_out": grad_out.astype(jnp.bfloat16)}


def block_pass(tok_rows, grad_rows, w_gate, w_up, w_down):
    gate_pre = jnp.dot(tok_rows, w_gate, preferred_element_type=jnp.float32).astype(jnp.bfloat16).astype(jnp.float32)
    up_pre = jnp.dot(tok_rows, w_up, preferred_element_type=jnp.float32).astype(jnp.bfloat16).astype(jnp.float32)
    gate_sig = jax.nn.sigmoid(gate_pre)
    silu_gate = gate_pre * gate_sig
    hidden = (silu_gate * up_pre).astype(jnp.bfloat16)
    down_out = jnp.dot(hidden, w_down, preferred_element_type=jnp.float32)
    out_rows = (tok_rows.astype(jnp.float32) + down_out).astype(jnp.bfloat16)
    grad_hidden = jnp.dot(grad_rows, w_down.T, preferred_element_type=jnp.float32).astype(jnp.bfloat16).astype(jnp.float32)
    grad_gate_pre = (grad_hidden * up_pre * gate_sig * (1.0 + gate_pre * (1.0 - gate_sig))).astype(jnp.bfloat16)
    grad_up_pre = (grad_hidden * silu_gate).astype(jnp.bfloat16)
    back_sum = jnp.dot(grad_gate_pre, w_gate.T, preferred_element_type=jnp.float32) + jnp.dot(grad_up_pre, w_up.T, preferred_element_type=jnp.float32)
    grad_in = (grad_rows.astype(jnp.float32) + back_sum).astype(jnp.bfloat16)
    part_gate = jnp.dot(tok_rows.T, grad_gate_pre, preferred_element_type=jnp.float32)
    part_up = jnp.dot(tok_rows.T, grad_up_pre, preferred_element_type=jnp.float32)
    part_down = jnp.dot(hidden.T, grad_rows, preferred_element_type=jnp.float32)
    return out_rows, grad_in, part_gate, part_up, part_down


def reference(tokens, w_gate, w_up, w_down, grad_out):
    block_count = TOKENS // BLOCK_ROWS
    tok_blocks = tokens.reshape(block_count, BLOCK_ROWS, D_MODEL)
    grad_blocks = grad_out.reshape(block_count, BLOCK_ROWS, D_MODEL)

    def scan_step(acc_carry, block_pair):
        acc_gate, acc_up, acc_down = acc_carry
        tok_rows, grad_rows = block_pair
        out_rows, grad_in, part_gate, part_up, part_down = block_pass(tok_rows, grad_rows, w_gate, w_up, w_down)
        return (acc_gate + part_gate, acc_up + part_up, acc_down + part_down), (out_rows, grad_in)

    zero_acc = (jnp.zeros((D_MODEL, D_FF), jnp.float32), jnp.zeros((D_MODEL, D_FF), jnp.float32), jnp.zeros((D_FF, D_MODEL), jnp.float32))
    acc_final, row_outs = lax.scan(scan_step, zero_acc, (tok_blocks, grad_blocks))
    grad_gate, grad_up, grad_down = acc_final
    out_blocks, grad_in_blocks = row_outs
    return (out_blocks.reshape(TOKENS, D_MODEL), grad_in_blocks.reshape(TOKENS, D_MODEL), grad_gate, grad_up, grad_down)
```

```python
import functools

import jax
import jax.numpy as jnp
from jax import lax
from jax.experimental import pallas as pl
from jax.experimental.pallas import tpu as pltpu
from jax.sharding import PartitionSpec as P

ROW_SPEC = P(("datb", "data", "model"), None)
GATE_SPEC = P(("datb", "data"), "model")
DOWN_SPEC = P("model", ("datb", "data"))
BF = jnp.bfloat16
F32 = jnp.float32
SWAP = ((0, 1), (1, 0))
VMEM_LIMIT = 62 * 1024 * 1024
CHUNKS = (512, 512, 1024, 1024, 1024, 1024, 1024, 512, 512)
SPLIT_FROM = 6
STEPS = {2: [("r", (0, 1, 2))], 3: [("w", (0, 1, 2))], 4: [("r", (3, 4))], 5: [("w", (3,))], 7: [("r", (5, 6, 7))], 8: [("r", (8,))]}
LAST = [(4, 5), (6, 7, 8)]


def swap(value, axis):
    return lax.ppermute(value, axis, SWAP)


def after(value, *others):
    return lax.optimization_barrier((value, *others))[0]


def dot(lhs, rhs, l_dim=1, r_dim=0):
    return lax.dot_general(lhs, rhs, (((l_dim,), (r_dim,)), ((), ())), preferred_element_type=F32)


def hidden_kernel(n_rows, idx_ref, *refs):
    x_blocks, dy_blocks = refs[:n_rows], refs[n_rows : 2 * n_rows]
    refs = refs[2 * n_rows :]
    wg, wu, wd = refs[0:4], refs[4:8], refs[8:12]
    h_ref, da_ref, db_ref, x_buf, dy_buf, sems = refs[-6:]
    d_part = wg[0].shape[0]
    i = pl.program_id(1)
    step = pl.program_id(0) * n_rows + i
    total = pl.num_programs(0) * n_rows
    slot = lax.rem(step, 2)

    def copies(r, s):
        return (
            pltpu.make_async_copy(x_blocks[r], x_buf.at[s], sems.at[0, s]),
            pltpu.make_async_copy(dy_blocks[r], dy_buf.at[s], sems.at[1, s]),
        )

    @pl.when(step == 0)
    def _():
        for c in copies(0, 0):
            c.start()

    for r in range(n_rows):

        @pl.when(jnp.logical_and(step + 1 < total, lax.rem(i + 1, n_rows) == r))
        def _():
            for c in copies(r, 1 - slot):
                c.start()

    for c in copies(0, slot):
        c.wait()
    a = b = g = None
    for p in range(4):
        col = pl.multiple_of(jnp.bitwise_xor(idx_ref[0], p) * d_part, d_part)
        x_p = x_buf[slot, :, pl.ds(col, d_part)]
        dy_p = dy_buf[slot, :, pl.ds(col, d_part)]
        a_p, b_p, g_p = dot(x_p, wg[p][...]), dot(x_p, wu[p][...]), dot(dy_p, wd[p][...], 1, 1)
        a = a_p if a is None else a + a_p
        b = b_p if b is None else b + b_p
        g = g_p if g is None else g + g_p
    a, b, g = (v.astype(BF).astype(F32) for v in (a, b, g))
    sig = jax.nn.sigmoid(a)
    silu = a * sig
    h_ref[...] = (silu * b).astype(BF)
    da_ref[...] = (g * b * sig * (1.0 + a * (1.0 - sig))).astype(BF)
    db_ref[...] = (g * silu).astype(BF)


def hidden_call(idx, x, dy, weights, start, size, deps=(), tf=512):
    gate, up, down = weights
    n_rows = len(x)
    tm, d_model = x[0].shape
    rows = tm * n_rows
    d_part = gate[0].shape[0]
    base = (start // tf, start // tf, 0, 0)
    any_spec = pl.BlockSpec(memory_space=pl.ANY)
    col_specs = [pl.BlockSpec((d_part, tf), lambda j, i, s, o=o: (0, j + o)) for o in base]
    down_specs = [pl.BlockSpec((tf, d_part), lambda j, i, s, o=o: (j + o, 0)) for o in base]
    out_spec = pl.BlockSpec((tm, tf), lambda j, i, s: (i, j))
    flops = 6 * rows * d_model * size
    return pl.pallas_call(
        functools.partial(hidden_kernel, n_rows),
        out_shape=[jax.ShapeDtypeStruct((rows, size), BF)] * 3,
        grid_spec=pltpu.PrefetchScalarGridSpec(
            num_scalar_prefetch=1,
            grid=(size // tf, n_rows),
            in_specs=[any_spec] * (2 * n_rows) + col_specs + col_specs + down_specs + [any_spec] * len(deps),
            out_specs=[out_spec] * 3,
            scratch_shapes=[pltpu.VMEM((2, tm, d_model), BF), pltpu.VMEM((2, tm, d_model), BF), pltpu.SemaphoreType.DMA((2, 2))],
        ),
        compiler_params=pltpu.CompilerParams(dimension_semantics=("arbitrary", "arbitrary"), vmem_limit_bytes=VMEM_LIMIT),
        cost_estimate=pl.CostEstimate(flops=flops, bytes_accessed=6 * d_model * size + 6 * rows * size, transcendentals=rows * size),
        name="hidden",
    )(idx, *x, *dy, *gate, *up, *down, *deps)


def rows_kernel(parts, first, *refs):
    groups = [refs[15 * k : 15 * k + 15] for k in range(parts)]
    y_out, dx_out = refs[-2:]
    for p in range(4):
        y = dx = None
        for grp in groups:
            y_k = dot(grp[0][...], grp[11 + p][...])
            dx_k = dot(grp[1][...], grp[3 + p][...], 1, 1) + dot(grp[2][...], grp[7 + p][...], 1, 1)
            y = y_k if y is None else y + y_k
            dx = dx_k if dx is None else dx + dx_k
        if not first:
            y = refs[15 * parts][p] + y
            dx = refs[15 * parts + 1][p] + dx
        y_out[p] = y
        dx_out[p] = dx


def rows_call(chunks, sums, deps=(), tn=256):
    d_part = chunks[0][3][0][0].shape[0]
    rows = 1024
    width = sum(c[5] for c in chunks)
    tm = 512 if width <= 2048 else 256
    sum_spec = pl.BlockSpec((4, tm, tn), lambda n, m: (0, m, n))
    any_spec = pl.BlockSpec(memory_space=pl.ANY)
    specs, operands = [], []
    for h, da, db, (gate, up, down), start, size in chunks:
        assert start % size == 0
        base = (start // size, start // size, 0, 0)
        specs += [pl.BlockSpec((tm, size), lambda n, m: (m, 0))] * 3
        specs += [pl.BlockSpec((tn, size), lambda n, m, o=o: (n, o)) for o in base] * 2
        specs += [pl.BlockSpec((size, tn), lambda n, m, o=o: (o, n)) for o in base]
        operands += [h, da, db, *gate, *up, *down]
    count = len(operands)
    first = sums is None
    if not first:
        specs += [sum_spec] * 2
        operands += list(sums)
    return pl.pallas_call(
        functools.partial(rows_kernel, len(chunks), first),
        out_shape=[jax.ShapeDtypeStruct((4, rows, d_part), F32)] * 2,
        grid=(d_part // tn, rows // tm),
        in_specs=specs + [any_spec] * len(deps),
        out_specs=[sum_spec] * 2,
        input_output_aliases={} if first else {count: 0, count + 1: 1},
        compiler_params=pltpu.CompilerParams(dimension_semantics=("arbitrary", "arbitrary"), vmem_limit_bytes=VMEM_LIMIT),
        cost_estimate=pl.CostEstimate(flops=24 * rows * d_part * width, bytes_accessed=24 * d_part * width + 64 * rows * d_part, transcendentals=0),
        name="rows",
    )(*operands, *deps)


def weight_kernel(layout, steps, x_refs, refs):
    x_own, x_peer, dy_own, dy_peer = x_refs
    gate_out, up_out, down_out = refs[-3:]
    j = pl.program_id(0)

    def term(lefts, pieces):
        total = None
        for (side, offset), ref in pieces:
            t = dot(lefts[side][:, pl.ds(offset, ref.shape[0])], ref[...])
            total = t if total is None else total + t
        return total

    pos = 0
    for k, places in enumerate(layout):
        n = len(places)
        h, da, db = (list(zip(places, refs[pos + q * n : pos + q * n + n])) for q in range(3))
        pos += 3 * n

        @pl.when(jnp.logical_and(j >= steps[k], j < steps[k + 1]))
        def _():
            gate_out[...] = term((x_own, x_peer), da)
            up_out[...] = term((x_own, x_peer), db)
            down_out[...] = term((dy_own, dy_peer), h).T


def weight_call(columns, chunks, outs, d_ff, deps=(), tf=256):
    d_part, half = columns[0].shape
    base = chunks[0][1] // tf
    full_spec = pl.BlockSpec((d_part, half), lambda j: (0, 0), pipeline_mode=pl.Buffered(1))
    any_spec = pl.BlockSpec(memory_space=pl.ANY)
    specs, operands, layout, steps = [], [], [], [0]
    for pieces, _, size in chunks:
        lo, n = steps[-1], size // tf
        layout.append([(side, offset) for side, offset, _ in pieces])
        for q in range(3):
            for _, _, values in pieces:
                specs.append(pl.BlockSpec((values[q].shape[0], tf), lambda j, lo=lo, n=n: (0, jnp.clip(j - lo, 0, n - 1))))
                operands.append(values[q])
        steps.append(lo + n)
    first = outs is None
    count = 4 + len(operands)
    width = steps[-1] * tf
    col_spec = pl.BlockSpec((d_part, tf), lambda j: (0, j + base))
    down_spec = pl.BlockSpec((tf, d_part), lambda j: (j + base, 0))

    def kernel(*refs):
        weight_kernel(layout, steps, refs[:4], refs[4:count] + refs[-3:])

    return pl.pallas_call(
        kernel,
        out_shape=[jax.ShapeDtypeStruct((d_part, d_ff), F32)] * 2 + [jax.ShapeDtypeStruct((d_ff, d_part), F32)],
        grid=(steps[-1],),
        in_specs=[full_spec] * 4 + specs + ([] if first else [any_spec] * 3) + [any_spec] * len(deps),
        out_specs=[col_spec, col_spec, down_spec],
        input_output_aliases={} if first else {count: 0, count + 1: 1, count + 2: 2},
        compiler_params=pltpu.CompilerParams(dimension_semantics=("arbitrary",), vmem_limit_bytes=VMEM_LIMIT),
        cost_estimate=pl.CostEstimate(flops=12 * half * d_part * width, bytes_accessed=12 * half * width + 12 * d_part * width, transcendentals=0),
        name="weights",
    )(*columns, *operands, *(() if first else outs), *deps)


def local_step(tok, wg, wu, wd, dy):
    rows_dev, d_model = tok.shape
    d_part, d_ff = wg.shape
    own = 2 * lax.axis_index("datb") + lax.axis_index("data")
    idx = jnp.reshape(own, (1,)).astype(jnp.int32)

    tok_y, dy_y = swap(tok, "datb"), swap(dy, "datb")
    tok_x, dy_x = swap(tok, "model"), swap(dy, "model")
    wg_c, wu_c, wd_c = swap(wg, "data"), swap(wu, "data"), swap(wd, "data")
    starts = [sum(CHUNKS[:k]) for k in range(len(CHUNKS))]
    sent = []
    for start, size in zip(starts, CHUNKS):
        part = slice(start, start + size)
        sent.append([swap(wg[:, part], "datb"), swap(wu[:, part], "datb"), swap(wd[part], "datb")])
    x = [tok, tok_x, tok_y, swap(tok_y, "model")]
    g = [dy, dy_x, dy_y, swap(dy_y, "model")]

    def columns(blocks):
        def cut(which):
            at = jnp.bitwise_xor(own, which) * d_part
            return jnp.concatenate([lax.dynamic_slice_in_dim(v, at, d_part, axis=1).T for v in blocks], axis=1)

        return cut(0), swap(cut(1), "data")

    cols = None
    sums = outs = None
    chunk_w, front, pieces = {}, {}, {}
    waiting = []
    token = ()

    def hidden(k, blocks, offset):
        nonlocal token
        lo, hi = blocks
        vals = hidden_call(idx, x[lo:hi], g[lo:hi], chunk_w[k], starts[k], CHUNKS[k], token)
        token = (vals[0],)
        moved = [swap(v, "data") for v in vals]
        pieces.setdefault(k, []).extend([(0, offset, vals), (1, offset, moved)])
        if lo == 0:
            front[k] = vals

    def add_rows(ks):
        nonlocal sums, token
        sums = rows_call([(*front[k], chunk_w[k], starts[k], CHUNKS[k]) for k in ks], sums, token)
        token = (sums[0],)

    def add_weights(ks):
        nonlocal outs, token, cols
        if cols is None:
            cols = [*columns(x), *columns(g)]
        outs = weight_call(cols, [(pieces[k], starts[k], CHUNKS[k]) for k in ks], outs, d_ff, token)
        token = (outs[0],)

    for k in range(len(CHUNKS)):
        arrived = [after(v, *token) for v in sent[k]]
        chunk_w[k] = tuple((own_w, peer_w, v, swap(v, "data")) for own_w, peer_w, v in zip((wg, wu, wd), (wg_c, wu_c, wd_c), arrived))
        if k < SPLIT_FROM:
            hidden(k, (0, 4), 0)
        else:
            hidden(k, (0, 2), 0)
            waiting.append(k)
        for kind, ks in STEPS.get(k, ()):
            (add_rows if kind == "r" else add_weights)(ks)

    def to_rows(part_sum, base):
        moved = swap(part_sum[:, rows_dev:].astype(BF), "model").astype(F32)
        total = part_sum[:, :rows_dev] + moved
        parts = [lax.dynamic_index_in_dim(total, jnp.bitwise_xor(own, q), 0, keepdims=False) for q in range(4)]
        return (base.astype(F32) + jnp.concatenate(parts, axis=1)).astype(BF)

    final = sums
    for k in waiting:
        hidden(k, (2, 4), 2 * rows_dev)
    for ks in LAST:
        add_weights(ks)
    return (to_rows(final[0], tok), to_rows(final[1], dy), *outs)


def solution(mesh):
    return jax.shard_map(local_step, mesh=mesh, in_specs=(ROW_SPEC, GATE_SPEC, GATE_SPEC, DOWN_SPEC, ROW_SPEC), out_specs=(ROW_SPEC, ROW_SPEC, GATE_SPEC, GATE_SPEC, DOWN_SPEC), check_vma=False)
```
